32 devices in a mesh: types: 4 (over y, x), inst: 2 (over core), face: 4 (over z).
Axes of the slice: x: 2, y: 2, z: 4, core: 2. Of those that a mesh axis runs over, the one named last changes fastest.
Arguments:
- coupling_modes: bfloat16 [8, 1024, 16384], P(('types', 'inst'), None, 'face'), may hold values from -0.0625 to 0.0625
- mode_stiffness: float32 [8, 16384], P(('types', 'inst'), 'face'), may hold values from 1 to 8
- boundary_stiffness: float32 [8, 1024, 1024], P(('types', 'inst'), 'face'), may hold values from -1 to 9, as said below
- slot_type: int32 [4, 2, 4, 2], P('types', 'inst', 'face'), may hold values from 0 to 1
- partner_slot: int32 [4, 2, 4, 3, 2], P('types', 'inst', 'face'), may hold values from 0 to 1, each once within a row
- port_map: int32 [4, 2, 4, 3, 2, 128], P('types', 'inst', 'face'), may hold values from 0 to 127, each once within a row
- loads: float32 [4, 2, 4, 2, 1024, 128], P('types', 'inst', 'face'), may hold values from -24 to 24
Outputs:
- displacement: float32 [4, 2, 4, 2, 1024, 128], P('types', 'inst', 'face')
The draws below stay inside these ranges and needn't reach their ends.
Inputs may be any that keep to these rules, and one draw needn't show every extreme that they name: `boundary_stiffness`: each type's matrix is symmetric.
All inputs are finite; a program needn't handle non-finite values.
Results may differ from the reference program's by a relative error of at most 0.004.
Values may be sent and summed in bfloat16 or wider, within the bound.
No kernel may reach another device: no remote copies, remote signals or barrier semaphores. Data moves between devices by JAX's collectives and lax.ppermute only.
A program may use at most 128 MiB of HBM per device.

```python
import math
import jax
import jax.numpy as jnp
import numpy as np
from jax import lax

NB = 1024
PORT = 128
MODES = 16384
TYPES = 8
SLOTS = 2
LOADS = 128
SWEEPS = 4
N_TYPES = 4
N_INST = 2
N_FACE = 4


def draw_boundary_stiffness(key, part):
    noise = jax.random.normal(key, (TYPES, NB, NB), jnp.float32)
    symmetric = (noise + jnp.swapaxes(noise, 1, 2)) / jnp.sqrt(2.0 * NB)
    return 7.0 * jnp.eye(NB, dtype=jnp.float32)[None, :, :] + symmetric


def place_ends(drawn, own_key, smallest, high):
    spot = [jax.random.randint(jax.random.fold_in(own_key, axis), (), 0, length) for axis, length in enumerate(drawn.shape)]
    widest = drawn.shape.index(max(drawn.shape))
    next_to = spot[:widest] + [(spot[widest] + 1) % drawn.shape[widest]] + spot[widest + 1:]
    return drawn.at[tuple(spot)].set(smallest).at[tuple(next_to)].set(high)


def spiked(values, stream_key, source, target, shards_of, factor):
    def block_of(position):
        return (jnp.arange(values.shape[position]) // (values.shape[position] // shards_of)).reshape((-1,) + (1,) * (values.ndim - 1 - position))

    one_side = jax.random.permutation(stream_key, shards_of)[block_of(target)]
    second = (block_of(target) + shards_of // 2) % shards_of
    return jnp.where((block_of(source) == one_side) | (block_of(source) == second), factor * values, values)


def level_of(key, shape, split, low, high):
    loudness = 1.0
    for dim, shards_of in split:
        heights = jax.random.uniform(jax.random.fold_in(jax.random.fold_in(key, 6), dim), (shards_of,), jnp.float32, low / len(split), high / len(split))
        loudness = loudness * jnp.repeat(jnp.exp(heights), shape[dim] // shards_of).reshape((-1,) + (1,) * (len(shape) - 1 - dim))
    return loudness


def cumulative_ranks(number_of, lean):
    weights = [(1 << 20) // math.isqrt(grade ** lean) + 1 for grade in range(1, number_of + 1)]
    spread = 1 + sum(weights) // (1 << 30)
    return np.cumsum(np.array([max(1, weight // spread) for weight in weights]))


def skewed_ids(rng, extent, count, lean):
    table = cumulative_ranks(count, lean)
    lot = jax.random.randint(jax.random.fold_in(rng, 1), extent, 0, int(table[count - 1]))
    grade = jnp.searchsorted(jnp.asarray(table, jnp.int32), lot, side="right")
    return jax.random.permutation(jax.random.fold_in(rng, 2), count)[grade].astype(jnp.int32)


def centred(stream_key, dims, spread, limit, split=(), held_as=jnp.bfloat16):
    values = jax.random.normal(stream_key, dims, jnp.float32) * spread
    if len(split) > 0:
        values = level_of(stream_key, dims, split, -0.22, 0.18) * values
    return jnp.clip(values, min=-limit, max=limit).astype(held_as)


def heavy_noise(rng, dims, spread, bound, pieces, heavy, held_as=jnp.bfloat16):
    array = spread * jax.random.normal(rng, dims, jnp.float32)
    if pieces:
        array = array * level_of(rng, dims, pieces, -0.22, 0.18)
    return jnp.clip(spiked(array, jax.random.fold_in(rng, 3), *heavy), -bound, bound).astype(held_as)


def setup_inputs(seed: int = 0) -> dict:
    key_of = jax.random.split(jax.random.key(seed), 8)
    coupling_modes = heavy_noise(key_of[0], (TYPES, NB, MODES), MODES ** -0.5, 0.0625, ((0, 8), (2, 4)), (2, 1, 4, 2.0))
    mode_stiffness = jnp.clip(jnp.exp(math.log(8.0) - 2.0794415 * jax.random.uniform(key_of[1], (TYPES, MODES), jnp.float32) ** level_of(key_of[1], (TYPES, MODES), ((0, 8), (1, 4)), -0.2, 0.2)), 1.0, 8.0)
    boundary_stiffness = draw_boundary_stiffness(jax.random.fold_in(key_of[7], 71), 0)
    slot_type = place_ends(skewed_ids(key_of[3], (N_TYPES, N_INST, N_FACE, SLOTS), N_INST, 2), jax.random.fold_in(key_of[3], 3), 0, N_INST - 1).astype(jnp.int32)
    partner_slot = jax.vmap(lambda own: jax.random.permutation(own, SLOTS))(jax.random.split(key_of[4], N_TYPES * N_INST * N_FACE * 3)).reshape((N_TYPES, N_INST, N_FACE, 3, SLOTS)).astype(jnp.int32)
    port_map = jax.vmap(lambda own: jax.random.permutation(own, PORT))(jax.random.split(key_of[5], N_TYPES * N_INST * N_FACE * 3 * SLOTS)).reshape((N_TYPES, N_INST, N_FACE, 3, SLOTS, PORT)).astype(jnp.int32)
    loads = centred(key_of[6], (N_TYPES, N_INST, N_FACE, SLOTS, NB, LOADS), 4.0, 24.0, ((0, 4), (1, 2), (2, 4)), jnp.float32)
    return {"coupling_modes": coupling_modes, "mode_stiffness": mode_stiffness, "boundary_stiffness": boundary_stiffness, "slot_type": slot_type, "partner_slot": partner_slot, "port_map": port_map, "loads": loads}


lower_bound = 2.0
upper_bound = 12.0


def fetch_ports(source, slot_ids, port_ids):
    return source[slot_ids[:, None], port_ids]


def place_ports(values, slot_ids, port_ids):
    return jnp.zeros_like(values).at[slot_ids[:, None], port_ids].set(values)


def over_grid(function):
    return jax.vmap(jax.vmap(jax.vmap(function)))


def shift_grid(values, grid_dim, offset):
    length = values.shape[grid_dim]
    padding = jnp.zeros_like(lax.slice_in_dim(values, 0, 1, axis=grid_dim))
    if offset > 0:
        kept = lax.slice_in_dim(values, 0, length - 1, axis=grid_dim)
        return jnp.concatenate([padding, kept], axis=grid_dim)
    kept = lax.slice_in_dim(values, 1, length, axis=grid_dim)
    return jnp.concatenate([kept, padding], axis=grid_dim)


def grid_masks(grid_dim):
    shape = (N_TYPES, N_INST, N_FACE, 1, 1, 1)
    positions = lax.broadcasted_iota(jnp.int32, shape, grid_dim)
    length = shape[grid_dim]
    return (positions < length - 1).astype(jnp.float32), (positions > 0).astype(jnp.float32)


def couple(values, partner_slot, port_map):
    terms = []
    for direction, grid_dim in ((0, 1), (1, 2), (2, 0)):
        upper_side = values[:, :, :, :, 2 * direction * PORT:(2 * direction + 1) * PORT]
        lower_side = values[:, :, :, :, (2 * direction + 1) * PORT:(2 * direction + 2) * PORT]
        slot_ids = partner_slot[:, :, :, direction]
        port_ids = port_map[:, :, :, direction]
        from_next = shift_grid(lower_side, grid_dim, -1)
        partner = over_grid(fetch_ports)(from_next, slot_ids, port_ids)
        outgoing = over_grid(place_ports)(upper_side, slot_ids, port_ids)
        from_prev = shift_grid(outgoing, grid_dim, 1)
        has_next, has_prev = grid_masks(grid_dim)
        terms.append(has_next * (upper_side - partner))
        terms.append(has_prev * (lower_side - from_prev))
    shape = values.shape
    terms.append(jnp.zeros(shape[:4] + (NB - 6 * PORT, shape[5]), jnp.float32))
    return jnp.concatenate(terms, axis=4)


def reference(coupling_modes, mode_stiffness, boundary_stiffness, slot_type, partner_slot, port_map, loads):
    def one_type(triple):
        modes, stiffness, boundary = triple
        scaled = (modes.astype(jnp.float32) / stiffness[None, :]).astype(jnp.bfloat16)
        partial_value = jnp.dot(scaled.astype(jnp.float32), modes.astype(jnp.float32).T, precision=lax.Precision.HIGHEST)
        return (boundary - partial_value).astype(jnp.bfloat16)

    blocks = lax.map(one_type, (coupling_modes, mode_stiffness, boundary_stiffness))
    group_index = lax.broadcasted_iota(jnp.int32, (N_TYPES, N_INST, N_FACE, SLOTS), 0)
    type_index = (group_index * N_INST + slot_type).reshape(-1).astype(jnp.int32)

    def one_product(pair):
        kind, vector = pair
        return jnp.dot(blocks[kind].astype(jnp.float32), vector.astype(jnp.float32), precision=lax.Precision.HIGHEST)

    def operator_apply(values):
        lowered = values.astype(jnp.bfloat16).reshape(-1, NB, LOADS)
        product = lax.map(one_product, (type_index, lowered)).reshape(values.shape)
        return product + couple(values, partner_slot, port_map)

    theta = (upper_bound + lower_bound) / 2.0
    delta = (upper_bound - lower_bound) / 2.0
    sigma = theta / delta
    weight_now = 1.0 / sigma
    displacement = jnp.zeros_like(loads)
    residual = loads
    direction = loads / theta
    for sweep_index in range(SWEEPS):
        displacement = displacement + direction
        residual = residual - operator_apply(direction)
        weight_next = 1.0 / (2.0 * sigma - weight_now)
        direction = (weight_next * weight_now) * direction + (2.0 * weight_next / delta) * residual
        weight_now = weight_next
    return displacement
```

```python
import jax
import jax.numpy as jnp
from jax import lax
from jax.experimental import pallas as pl
from jax.experimental.pallas import tpu as pltpu
from jax.sharding import PartitionSpec as P

SIDES = 8
lower_bound = 2.0
upper_bound = 12.0
theta = (upper_bound + lower_bound) / 2.0
delta = (upper_bound - lower_bound) / 2.0
sigma = theta / delta
w0 = 1.0 / sigma
w1 = 1.0 / (2.0 * sigma - w0)
w2 = 1.0 / (2.0 * sigma - w1)
w3 = 1.0 / (2.0 * sigma - w2)
keep = (w1 * w0, w2 * w1, w3 * w2)
gain = (2.0 * w1 / delta, 2.0 * w2 / delta, 2.0 * w3 / delta)

AXES = ("inst", "face", "types")
F32 = jnp.float32
BF16 = jnp.bfloat16
VMEM = pl.BlockSpec(memory_space=pltpu.VMEM)
SMEM = pl.BlockSpec(memory_space=pltpu.SMEM)


def dot(a, b):
    return lax.dot_general(a, b, (((1,), (0,)), ((), ())), preferred_element_type=F32)


def dot_nt(a, b):
    return lax.dot_general(a, b, (((1,), (1,)), ((), ())), preferred_element_type=F32)


def shape_of(dims, dtype):
    return jax.ShapeDtypeStruct(dims, dtype)


def call(body, out_shape, operands, specs, flops, name):
    moved = sum(x.size * x.dtype.itemsize for x in operands)
    return pl.pallas_call(
        body,
        out_shape=out_shape,
        in_specs=specs,
        out_specs=jax.tree.map(lambda _: VMEM, out_shape),
        cost_estimate=pl.CostEstimate(flops=flops, bytes_accessed=moved, transcendentals=0),
        name=name,
    )(*operands)


def owned_boundary(bd_ref, row, count, face):
    held = bd_ref.shape[0]
    step = min(held, count)
    parts = []
    for start in range(row, row + count, step):
        local = bd_ref[start % held : start % held + step, :]
        parts.append(jnp.where(face == start // held, local, 0.0))
    return parts[0] if len(parts) == 1 else jnp.concatenate(parts, axis=0)


def modal_blocks(modes, stiffness, boundary, pairs, packed, name):
    nb, depth = modes.shape
    block = 2 * nb // SIDES
    half = block // 2
    count = nb // block
    tile = min(1024, depth)
    steps = depth // tile
    rows = sorted({i for pair in pairs for i in pair})
    lefts = sorted({i for i, _ in pairs})
    if packed:
        height = half * ((count + 1) // 2)
        extra = 16 * ((2 * count + 15) // 16)
        out_rows = 2 * height + extra
    else:
        out_rows = block * len(pairs)

    def body(*refs):
        k_ref = refs[0]
        c_refs = dict(zip(rows, refs[1 : 1 + len(rows)]))
        b_refs = refs[1 + len(rows) : 1 + len(rows) + len(pairs)]
        out_ref, acc_ref = refs[-2:]
        step = pl.program_id(0)
        inverse = 1.0 / k_ref[...]
        left = {i: (c_refs[i][...].astype(F32) * inverse).astype(BF16) for i in lefts}
        for n, (i, j) in enumerate(pairs):
            part = dot_nt(left[i], c_refs[j][...])

            @pl.when(step == 0)
            def _():
                acc_ref[n] = part

            @pl.when(step > 0)
            def _():
                acc_ref[n] += part

        @pl.when(step == steps - 1)
        def _():
            face = lax.axis_index("face")
            if not packed:
                for n, (i, j) in enumerate(pairs):
                    held = owned_boundary(b_refs[n], i * block, block, face)
                    out_ref[n * block : (n + 1) * block, :] = (held - acc_ref[n]).astype(BF16)
                return
            r = lax.broadcasted_iota(jnp.int32, (half, half), 0)
            c = lax.broadcasted_iota(jnp.int32, (half, half), 1)
            rr = lax.broadcasted_iota(jnp.int32, (block, block), 0)
            cc = lax.broadcasted_iota(jnp.int32, (block, block), 1)
            highs, rests = [], []
            for n, (i, _) in enumerate(pairs):
                held = owned_boundary(b_refs[n], i * block, block, face)
                acc = acc_ref[n]
                diff = held - acc
                own = jnp.sum(jnp.where(rr == cc, held, 0.0), axis=0, keepdims=True)
                modal = jnp.sum(jnp.where(rr == cc, acc, 0.0), axis=0, keepdims=True)
                high = own.astype(BF16).astype(F32)
                highs.append(high)
                rests.append((own - high) - modal)
                a = diff[:half, :half]
                b = diff[half:, half:]
                both = jnp.where(r < c, a, jnp.where(r > c, b, 0.0))
                top, side = half * (n // 2), half * (n % 2)
                out_ref[top : top + half, side : side + half] = both.astype(BF16)
                out_ref[height + top : height + top + half, side : side + half] = diff[
                    :half, half:
                ].astype(BF16)
            fill = [jnp.zeros((extra - 2 * count, block), F32)] if extra > 2 * count else []
            out_ref[2 * height :, :] = jnp.concatenate(highs + rests + fill, axis=0).astype(BF16)

    def row_spec(i):
        return pl.BlockSpec((block, tile), lambda k, i=i: (i, k))

    def boundary_spec(j):
        return pl.BlockSpec((boundary.shape[0], block), lambda k, j=j: (0, j))

    return pl.pallas_call(
        body,
        grid=(steps,),
        out_shape=shape_of((out_rows, block), BF16),
        in_specs=[pl.BlockSpec((1, tile), lambda k: (0, k))]
        + [row_spec(i) for i in rows]
        + [boundary_spec(j) for _, j in pairs],
        out_specs=pl.BlockSpec((out_rows, block), lambda k: (0, 0)),
        scratch_shapes=[pltpu.VMEM((len(pairs), block, block), F32)],
        cost_estimate=pl.CostEstimate(
            flops=2 * len(pairs) * block * block * depth,
            bytes_accessed=2 * len(rows) * block * depth,
            transcendentals=0,
        ),
        name=name,
    )(stiffness, *([modes] * len(rows)), *([boundary] * len(pairs)))


def unpack_diagonal(packed_list, count):
    block = packed_list[0].shape[1]
    half = block // 2
    height = half * ((count + 1) // 2)

    def body(*refs):
        total = len(refs) // 2
        r = lax.broadcasted_iota(jnp.int32, (half, half), 0)
        c = lax.broadcasted_iota(jnp.int32, (half, half), 1)
        for p_ref, d_ref in zip(refs[:total], refs[total:]):
            lines = p_ref[2 * height :, :].astype(F32)
            for i in range(count):
                line = lines[i : i + 1, :] + lines[count + i : count + i + 1, :]
                top, side = half * (i // 2), half * (i % 2)
                both = p_ref[top : top + half, side : side + half].astype(F32)
                off = p_ref[height + top : height + top + half, side : side + half]
                upper = jnp.where(r < c, both, 0.0)
                lower = jnp.where(r > c, both, 0.0)
                a = upper + upper.T + jnp.where(r == c, line[:, :half], 0.0)
                b = lower + lower.T + jnp.where(r == c, line[:, half:], 0.0)
                d_ref[i, :half, :half] = a.astype(BF16)
                d_ref[i, half:, half:] = b.astype(BF16)
                d_ref[i, :half, half:] = off
                d_ref[i, half:, :half] = off.astype(F32).T.astype(BF16)

    return call(
        body,
        [shape_of((count, block, block), BF16) for _ in packed_list],
        packed_list,
        [VMEM] * len(packed_list),
        10_000_000,
        "unpack_diagonal",
    )


def parity_and_masks(axis):
    index = lax.axis_index(axis)
    return index % 2 == 0, index < lax.axis_size(axis) - 1, index > 0


def side_pair(values, e, port):
    upper = [v[:, 2 * e * port : (2 * e + 1) * port] for v in values]
    lower = [v[:, (2 * e + 1) * port : (2 * e + 2) * port] for v in values]
    return jnp.concatenate(upper, axis=1), jnp.concatenate(lower, axis=1)


def write_sends(values, port, match_ref, send_refs):
    at = 0
    for e, axis in enumerate(AXES):
        even, _, _ = parity_and_masks(axis)
        upper, lower = side_pair(values, e, port)
        outgoing = dot_nt(upper.astype(BF16), match_ref[e])
        lower = lower.astype(BF16).astype(F32)
        send_refs[at][...] = jnp.where(even, outgoing, lower).astype(BF16)
        at += 1
        if lax.axis_size(axis) > 2:
            send_refs[at][...] = jnp.where(even, lower, outgoing).astype(BF16)
            at += 1


def arrivals(recv_refs):
    at = 0
    out = []
    for axis in AXES:
        even, has_next, has_prev = parity_and_masks(axis)
        first = recv_refs[at][...].astype(F32)
        at += 1
        if lax.axis_size(axis) > 2:
            second = recv_refs[at][...].astype(F32)
            at += 1
            after, before = jnp.where(even, first, second), jnp.where(even, second, first)
        else:
            after, before = first, first
        after = jnp.where(has_next, after, 0.0)
        before = jnp.where(has_prev, before, 0.0)
        out.append((after, before, has_next, has_prev))
    return out


def exchange(sends):
    at = 0
    out = []
    for axis in AXES:
        size = lax.axis_size(axis)
        for first in (0, 1) if size > 2 else (0,):
            swaps = []
            for p in range(first, size - 1, 2):
                swaps += [(p, p + 1), (p + 1, p)]
            out.append(lax.ppermute(sends[at], axis, swaps))
            at += 1
    return out


def send_shapes(load_count, width):
    total = sum(2 if lax.axis_size(axis) > 2 else 1 for axis in AXES)
    return [shape_of((load_count, width), BF16) for _ in range(total)]


def own_terms(values, port):
    sides = []
    for axis in AXES:
        _, has_next, has_prev = parity_and_masks(axis)
        sides += [has_next, has_prev]
    out = []
    for v in values:
        parts = [
            jnp.where(sides[k], v[:, k * port : (k + 1) * port], 0.0) for k in range(len(sides))
        ]
        parts.append(jnp.zeros((v.shape[0], v.shape[1] - len(sides) * port), F32))
        out.append(jnp.concatenate(parts, axis=1))
    return out


def arrival_terms(recv_refs, match_ref, slot_total, port, nb):
    parts = [[] for _ in range(slot_total)]
    for e, (after, before, _, _) in enumerate(arrivals(recv_refs)):
        partner = dot(after.astype(BF16), match_ref[e])
        for s in range(slot_total):
            parts[s] += [partner[:, s * port : (s + 1) * port], before[:, s * port : (s + 1) * port]]
    out = []
    for s in range(slot_total):
        rest = nb - 2 * len(AXES) * port
        parts[s].append(jnp.zeros((parts[s][0].shape[0], rest), F32))
        out.append(jnp.concatenate(parts[s], axis=1))
    return out


def per_device(
    coupling_modes, mode_stiffness, boundary_stiffness, slot_type, partner_slot, port_map, loads
):
    modes = coupling_modes[0]
    nb = modes.shape[0]
    boundary = boundary_stiffness[0]
    rhs = loads[0, 0, 0]
    slot_total, _, load_count = rhs.shape
    kinds = slot_type[0, 0, 0]
    partners = partner_slot[0, 0, 0]
    ports = port_map[0, 0, 0]
    port = nb // SIDES
    block = 2 * port
    count = nb // block
    width = slot_total * port
    insts = lax.axis_size("inst")
    faces = lax.axis_size("face")
    vec = (slot_total, load_count, nb)

    def prepare(loads_ref, partner_ref, ports_ref, b_ref, match_ref, back_ref, *send_refs):
        values = []
        for s in range(slot_total):
            b = loads_ref[s].T
            b_ref[s] = b
            values.append(b / theta)
        row = lax.broadcasted_iota(jnp.int32, (width, width), 0)
        for e in range(len(AXES)):
            target = jnp.concatenate(
                [partner_ref[e, s] * port + ports_ref[e, s : s + 1, :] for s in range(slot_total)],
                axis=1,
            )
            table = (row == target).astype(F32)
            match_ref[e] = table.astype(BF16)
            back_ref[e] = table.T.astype(BF16)
        write_sends(values, port, match_ref, send_refs)

    tables = shape_of((len(AXES), width, width), BF16)
    bt, match, back, *sends = call(
        prepare,
        [shape_of(vec, F32), tables, tables] + send_shapes(load_count, width),
        (rhs, partners, ports),
        [VMEM, SMEM, VMEM],
        200_000_000,
        "prepare",
    )

    stiffness = mode_stiffness[0][None, :]
    offs = [(i, j) for j in range(count) for i in range(j)]
    diag = [(i, i) for i in range(count)]
    middle = offs[1:-1]
    plan = [(offs[:1], False), (diag, True)]
    plan += [(middle[k : k + 2], False) for k in range(0, len(middle), 2)]
    plan += [(offs[-1:], False)]
    partial_sums = [
        modal_blocks(modes, stiffness, boundary, pairs, packed, f"modal_{n}")
        for n, (pairs, packed) in enumerate(plan)
    ]

    def add(a, b):
        return (a.astype(F32) + b.astype(F32)).astype(BF16)

    def over_faces(part):
        if faces != 4:
            return lax.psum(part.astype(F32), "face").astype(BF16)
        z = lax.axis_index("face")
        inner = (z == 1) | (z == 2)
        left = add(part, lax.ppermute(part, "face", [(0, 1), (3, 2)]))
        total = add(left, lax.ppermute(left, "face", [(1, 2), (2, 1)]))
        spread = lax.ppermute(total, "face", [(1, 0), (2, 3)])
        return jnp.where(inner, total, spread)

    summed = [over_faces(part) for part in partial_sums]

    if insts == 2:
        candidates = [(own, lax.ppermute(own, "inst", [(0, 1), (1, 0)])) for own in summed]
    else:
        candidates = []
        for own in summed:
            stack = lax.all_gather(own, "inst", axis=0)
            candidates.append(
                tuple(
                    lax.dynamic_index_in_dim(stack, kinds[s], 0, keepdims=False)
                    for s in range(slot_total)
                )
            )
    options = len(candidates[0])
    candidates[1] = tuple(unpack_diagonal(list(candidates[1]), count))

    def each_option(kind_ref, use):
        me = lax.axis_index("inst")
        for s in range(slot_total):
            for option in range(options):
                if insts == 2:
                    hit = (kind_ref[s] == me) if option == 0 else (kind_ref[s] != me)
                    pl.when(hit)(lambda s=s, option=option: use(s, option))
                elif option == s:
                    use(s, option)

    def products(x, chunk_ids, chunk_refs):
        acc = [None] * count

        def gather(j, v):
            acc[j] = v if acc[j] is None else acc[j] + v

        cols = [x[:, i * block : (i + 1) * block] for i in range(count)]
        for n, ref in zip(chunk_ids, chunk_refs):
            pairs, packed = plan[n]
            for at, (i, j) in enumerate(pairs):
                if packed:
                    gather(i, dot(cols[i], ref[i]))
                else:
                    matrix = ref[at * block : (at + 1) * block, :]
                    gather(j, dot(cols[i], matrix))
                    gather(i, dot_nt(cols[j], matrix))
        return acc

    everything = list(range(len(plan)))
    flops_all = 2 * slot_total * load_count * nb * nb

    def matrices(ids):
        return [candidates[n][o] for o in range(options) for n in ids]

    def option_refs(refs, ids, option):
        return refs[option * len(ids) : (option + 1) * len(ids)]

    received = exchange(sends)

    def couple_first(b_ref, match_ref, *refs):
        out_ref = refs[-1]
        values = [b_ref[s] / theta for s in range(slot_total)]
        mine = own_terms(values, port)
        theirs = arrival_terms(refs[:-1], match_ref, slot_total, port, nb)
        for s in range(slot_total):
            out_ref[s] = b_ref[s] - mine[s] + theirs[s]

    r1_base = call(
        couple_first,
        shape_of(vec, F32),
        (bt, match, *received),
        [VMEM] * (2 + len(received)),
        50_000_000,
        "couple_first",
    )

    early, late = everything[:-1], everything[-1:]

    def first_product(b_ref, r_ref, kind_ref, *refs):
        out_ref = refs[-1]

        def use(s, option):
            x = (b_ref[s] / theta).astype(BF16)
            acc = products(x, early, option_refs(refs, early, option))
            for j in range(count):
                cols = slice(j * block, (j + 1) * block)
                out_ref[s, :, cols] = r_ref[s, :, cols] - acc[j]

        each_option(kind_ref, use)

    mats = matrices(early)
    r1_part = call(
        first_product,
        shape_of(vec, F32),
        (bt, r1_base, kinds, *mats),
        [VMEM, VMEM, SMEM] + [VMEM] * len(mats),
        flops_all,
        "first_product",
    )

    def first_finish(b_ref, r_ref, match_ref, kind_ref, *refs):
        refs, (r_out, d_out), send_refs = (
            refs[: options * len(late)],
            refs[options * len(late) : options * len(late) + 2],
            refs[options * len(late) + 2 :],
        )

        def use(s, option):
            x = (b_ref[s] / theta).astype(BF16)
            acc = products(x, late, option_refs(refs, late, option))
            for j in range(count):
                cols = slice(j * block, (j + 1) * block)
                r = r_ref[s, :, cols]
                if acc[j] is not None:
                    r = r - acc[j]
                r_out[s, :, cols] = r
                d_out[s, :, cols] = keep[0] * (b_ref[s, :, cols] / theta) + gain[0] * r

        each_option(kind_ref, use)
        write_sends([d_out[s] for s in range(slot_total)], port, match_ref, send_refs)

    mats = matrices(late)
    r1, d1, *sends = call(
        first_finish,
        [shape_of(vec, F32), shape_of(vec, F32)] + send_shapes(load_count, width),
        (bt, r1_part, match, kinds, *mats),
        [VMEM, VMEM, VMEM, SMEM] + [VMEM] * len(mats),
        flops_all // 4,
        "first_finish",
    )

    received = exchange(sends)
    mats = matrices(everything)

    def second_product(d_ref, r_ref, kind_ref, *refs):
        out_ref = refs[-1]

        def use(s, option):
            d = d_ref[s]
            acc = products(d.astype(BF16), everything, option_refs(refs, everything, option))
            base = r_ref[s] - own_terms([d], port)[0]
            for j in range(count):
                cols = slice(j * block, (j + 1) * block)
                out_ref[s, :, cols] = base[:, cols] - acc[j]

        each_option(kind_ref, use)

    r2_base = call(
        second_product,
        shape_of(vec, F32),
        (d1, r1, kinds, *mats),
        [VMEM, VMEM, SMEM] + [VMEM] * len(mats),
        flops_all,
        "second_product",
    )

    def second_finish(d_ref, r_ref, match_ref, *refs):
        total = len(received)
        recv_refs, r_out, d_out, send_refs = (
            refs[:total],
            refs[total],
            refs[total + 1],
            refs[total + 2 :],
        )
        theirs = arrival_terms(recv_refs, match_ref, slot_total, port, nb)
        values = []
        for s in range(slot_total):
            r = r_ref[s] + theirs[s]
            d = keep[1] * d_ref[s] + gain[1] * r
            r_out[s] = r
            d_out[s] = d
            values.append(d)
        write_sends(values, port, match_ref, send_refs)

    r2, d2, *sends = call(
        second_finish,
        [shape_of(vec, F32), shape_of(vec, F32)] + send_shapes(load_count, width),
        (d1, r2_base, match, *received),
        [VMEM] * (3 + len(received)),
        100_000_000,
        "second_finish",
    )

    received = exchange(sends)

    def third_product(b_ref, d1_ref, d_ref, r_ref, kind_ref, *refs):
        out_ref = refs[-1]

        def use(s, option):
            d = d_ref[s]
            acc = products(d.astype(BF16), everything, option_refs(refs, everything, option))
            base = r_ref[s] - own_terms([d], port)[0]
            sums = (b_ref[s] / theta + d1_ref[s]) + d
            for j in range(count):
                cols = slice(j * block, (j + 1) * block)
                last = keep[2] * d[:, cols] + gain[2] * (base[:, cols] - acc[j])
                out_ref[s, cols, :] = (sums[:, cols] + last).T

        each_option(kind_ref, use)

    x_base = call(
        third_product,
        shape_of(rhs.shape, F32),
        (bt, d1, d2, r2, kinds, *mats),
        [VMEM] * 4 + [SMEM] + [VMEM] * len(mats),
        flops_all,
        "third_product",
    )

    def third_finish(x_ref, back_ref, *refs):
        out_ref = refs[-1]
        row = lax.broadcasted_iota(jnp.int32, (width, width), 0)
        col = lax.broadcasted_iota(jnp.int32, (width, width), 1)
        unit = (row == col).astype(F32).astype(BF16)
        for e, (after, before, _, _) in enumerate(arrivals(refs[:-1])):
            partner = dot_nt(back_ref[e], after.astype(BF16))
            behind = dot_nt(unit, before.astype(BF16))
            for s in range(slot_total):
                for side, term in ((2 * e, partner), (2 * e + 1, behind)):
                    rows = slice(side * port, (side + 1) * port)
                    out_ref[s, rows, :] = (
                        x_ref[s, rows, :] + gain[2] * term[s * port : (s + 1) * port]
                    )
        for s in range(slot_total):
            rows = slice(2 * len(AXES) * port, nb)
            out_ref[s, rows, :] = x_ref[s, rows, :]

    displacement = call(
        third_finish,
        shape_of(rhs.shape, F32),
        (x_base, back, *received),
        [VMEM] * (2 + len(received)),
        100_000_000,
        "third_finish",
    )
    return displacement[None, None, None]


def solution(mesh):
    placed = (
        P(("types", "inst"), None, "face"),
        P(("types", "inst"), "face"),
        P(("types", "inst"), "face", None),
        P("types", "inst", "face", None),
        P("types", "inst", "face", None, None),
        P("types", "inst", "face", None, None, None),
        P("types", "inst", "face", None, None, None),
    )
    return jax.shard_map(
        per_device,
        mesh=mesh,
        in_specs=placed,
        out_specs=P("types", "inst", "face", None, None, None),
        check_vma=False,
    )
```

```python
import jax
import jax.numpy as jnp
from jax import lax
from jax.experimental import pallas as pl
from jax.experimental.pallas import tpu as pltpu
from jax.sharding import PartitionSpec as P

SIDES = 8
lower_bound = 2.0
upper_bound = 12.0
theta = (upper_bound + lower_bound) / 2.0
delta = (upper_bound - lower_bound) / 2.0
sigma = theta / delta
w0 = 1.0 / sigma
w1 = 1.0 / (2.0 * sigma - w0)
w2 = 1.0 / (2.0 * sigma - w1)
w3 = 1.0 / (2.0 * sigma - w2)
keep = (w1 * w0, w2 * w1, w3 * w2)
gain = (2.0 * w1 / delta, 2.0 * w2 / delta, 2.0 * w3 / delta)

AXES = ("inst", "face", "types")
F32 = jnp.float32
BF16 = jnp.bfloat16
VMEM = pl.BlockSpec(memory_space=pltpu.VMEM)
ANY = pl.BlockSpec(memory_space=pl.ANY)
HBM = pl.BlockSpec(memory_space=pltpu.HBM)
LIMIT = 12 * 2**20
GRANT = 61 * 2**20
SMEM = pl.BlockSpec(memory_space=pltpu.SMEM)


def dot(a, b):
    return lax.dot_general(a, b, (((1,), (0,)), ((), ())), preferred_element_type=F32)


def dot_nt(a, b):
    return lax.dot_general(a, b, (((1,), (1,)), ((), ())), preferred_element_type=F32)


def shape_of(dims, dtype):
    return jax.ShapeDtypeStruct(dims, dtype)


def call(body, out_shape, operands, specs, flops, name):
    moved = sum(x.size * x.dtype.itemsize for x in operands)
    return pl.pallas_call(
        body,
        out_shape=out_shape,
        in_specs=specs,
        out_specs=jax.tree.map(lambda _: VMEM, out_shape),
        cost_estimate=pl.CostEstimate(flops=flops, bytes_accessed=moved, transcendentals=0),
        compiler_params=pltpu.CompilerParams(vmem_limit_bytes=LIMIT),
        name=name,
    )(*operands)


def owned_boundary(b_ref, row, height, col, width, face):
    held = b_ref.shape[0]
    step = min(held, height)
    parts = []
    for start in range(row, row + height, step):
        local = b_ref[start % held : start % held + step, col : col + width]
        parts.append(jnp.where(face == start // held, local, 0.0))
    return parts[0] if len(parts) == 1 else jnp.concatenate(parts, axis=0)


def modal_blocks(modes, stiffness, boundary, chunks, after, name):
    nb, depth = modes.shape
    block = 2 * nb // SIDES
    half = block // 2
    count = nb // block
    ktile = block
    load = min(1024, depth)
    loads = depth // load
    every = [pair for pairs, _ in chunks for pair in pairs]
    rows = sorted({i for pair in every for i in pair})
    lefts = sorted({i for i, _ in every})
    phases = []
    for at, (pairs, _) in enumerate(chunks):
        if phases and sum(len(chunks[n][0]) for n in phases[-1]) + len(pairs) <= count:
            phases[-1].append(at)
        else:
            phases.append([at])
    most = max(sum(len(chunks[n][0]) for n in phase) for phase in phases)
    height = half * ((count + 1) // 2)
    extra = 16 * ((2 * count + 15) // 16)
    out_shapes = [
        shape_of((2 * height + extra if packed else block * len(pairs), block), BF16)
        for pairs, packed in chunks
    ]

    def body(modes_ref, stiff_ref, bound_ref, *refs):
        outs = refs[len(after) : len(after) + len(chunks)]
        row_ref, left_ref, inverse, b_ref, sems = refs[len(after) + len(chunks) :]
        stiff_copy = pltpu.make_async_copy(stiff_ref, inverse, sems.at[0])
        bound_copy = pltpu.make_async_copy(bound_ref, b_ref, sems.at[1])
        stiff_copy.start()
        copies = {}
        for n in range(loads):
            cols = pl.ds(n * load, load)
            for at, i in enumerate(rows):
                copies[i, n] = pltpu.make_async_copy(
                    modes_ref.at[pl.ds(i * block, block), cols],
                    row_ref.at[at, :, cols],
                    sems.at[2 + n * len(rows) + at],
                )
                copies[i, n].start()
        bound_copy.start()
        stiff_copy.wait()
        inverse[...] = 1.0 / inverse[...]
        face = lax.axis_index("face")
        scaled_done = set()

        def multiply(*accs):
            for phase in phases:
                pairs = [pair for n in phase for pair in chunks[n][0]]
                columns = sorted({j for _, j in pairs})
                for n in range(depth // ktile):
                    cols = pl.ds(n * ktile, ktile)
                    for i in sorted({i for pair in pairs for i in pair}):
                        copy = copies.pop((i, n * ktile // load), None)
                        if copy is not None:
                            copy.wait()
                    for i in sorted({i for i, _ in pairs}):
                        if (i, n) not in scaled_done:
                            scaled_done.add((i, n))
                            value = row_ref[rows.index(i), :, cols].astype(F32)
                            left_ref[lefts.index(i), :, cols] = (
                                value * inverse[:, cols]
                            ).astype(BF16)
                    q = n % 2
                    for at, j in enumerate(columns):
                        register = (n // 2 * len(columns) + at) % 2
                        pltpu.matmul_push_rhs(
                            row_ref[rows.index(j), :, cols],
                            staging_register=register,
                            mxu_index=q,
                            transpose=True,
                        )
                        fresh = register
                        for m, (i, jj) in enumerate(pairs):
                            if jj == j:
                                pltpu.matmul_acc_lhs(
                                    accs[2 * m + q],
                                    left_ref[lefts.index(i), :, cols],
                                    load_staged_rhs=fresh,
                                )
                                fresh = None
                if phase[0] == 0:
                    bound_copy.wait()
                sums = [
                    pltpu.matmul_pop(accs[2 * m]) + pltpu.matmul_pop(accs[2 * m + 1])
                    for m in range(len(pairs))
                ]
                for n in phase:
                    own_pairs, packed = chunks[n]
                    write = write_packed if packed else write_plain
                    write(outs[n], own_pairs, sums[: len(own_pairs)])
                    sums = sums[len(own_pairs) :]

        def write_plain(out_ref, pairs, sums):
            for n, (i, j) in enumerate(pairs):
                mine = owned_boundary(b_ref, i * block, block, j * block, block, face)
                out_ref[n * block : (n + 1) * block, :] = (mine - sums[n]).astype(BF16)

        def write_packed(out_ref, pairs, sums):
            r = lax.broadcasted_iota(jnp.int32, (half, half), 0)
            c = lax.broadcasted_iota(jnp.int32, (half, half), 1)
            rr = lax.broadcasted_iota(jnp.int32, (block, block), 0)
            cc = lax.broadcasted_iota(jnp.int32, (block, block), 1)
            highs, rests = [], []
            for n, (i, _) in enumerate(pairs):
                mine = owned_boundary(b_ref, i * block, block, i * block, block, face)
                acc = sums[n]
                diff = mine - acc
                own = jnp.sum(jnp.where(rr == cc, mine, 0.0), axis=0, keepdims=True)
                modal = jnp.sum(jnp.where(rr == cc, acc, 0.0), axis=0, keepdims=True)
                high = own.astype(BF16).astype(F32)
                highs.append(high)
                rests.append((own - high) - modal)
                a = diff[:half, :half]
                b = diff[half:, half:]
                both = jnp.where(r < c, a, jnp.where(r > c, b, 0.0))
                top, side = half * (n // 2), half * (n % 2)
                out_ref[top : top + half, side : side + half] = both.astype(BF16)
                out_ref[height + top : height + top + half, side : side + half] = diff[
                    :half, half:
                ].astype(BF16)
            fill = [jnp.zeros((extra - 2 * count, block), F32)] if extra > 2 * count else []
            out_ref[2 * height :, :] = jnp.concatenate(highs + rests + fill, axis=0).astype(BF16)

        pl.run_scoped(
            multiply, *[pltpu.ACC(q)((block, block), F32) for _ in range(most) for q in (0, 1)]
        )

    return pl.pallas_call(
        body,
        out_shape=out_shapes,
        in_specs=[ANY] * (3 + len(after)),
        out_specs=[VMEM] * len(chunks),
        scratch_shapes=[
            pltpu.VMEM((len(rows), block, depth), BF16),
            pltpu.VMEM((len(lefts), block, depth), BF16),
            pltpu.VMEM((1, depth), F32),
            pltpu.VMEM(boundary.shape, F32),
            pltpu.SemaphoreType.DMA((2 + loads * len(rows),)),
        ],
        cost_estimate=pl.CostEstimate(
            flops=2 * len(every) * block * block * depth,
            bytes_accessed=2 * len(rows) * block * depth,
            transcendentals=0,
        ),
        compiler_params=pltpu.CompilerParams(vmem_limit_bytes=GRANT),
        name=name,
    )(modes, stiffness, boundary, *after)


def unpack_diagonal(packed_list, count):
    block = packed_list[0].shape[1]
    half = block // 2
    height = half * ((count + 1) // 2)

    def body(*refs):
        total = len(refs) // 2
        r = lax.broadcasted_iota(jnp.int32, (half, half), 0)
        c = lax.broadcasted_iota(jnp.int32, (half, half), 1)
        for p_ref, d_ref in zip(refs[:total], refs[total:]):
            lines = p_ref[2 * height :, :].astype(F32)
            for i in range(count):
                line = lines[i : i + 1, :] + lines[count + i : count + i + 1, :]
                top, side = half * (i // 2), half * (i % 2)
                both = p_ref[top : top + half, side : side + half].astype(F32)
                off = p_ref[height + top : height + top + half, side : side + half]
                upper = jnp.where(r < c, both, 0.0)
                lower = jnp.where(r > c, both, 0.0)
                a = upper + upper.T + jnp.where(r == c, line[:, :half], 0.0)
                b = lower + lower.T + jnp.where(r == c, line[:, half:], 0.0)
                d_ref[i, :half, :half] = a.astype(BF16)
                d_ref[i, half:, half:] = b.astype(BF16)
                d_ref[i, :half, half:] = off
                d_ref[i, half:, :half] = off.astype(F32).T.astype(BF16)

    return call(
        body,
        [shape_of((count, block, block), BF16) for _ in packed_list],
        packed_list,
        [VMEM] * len(packed_list),
        10_000_000,
        "unpack_diagonal",
    )


def parity_and_masks(axis):
    index = lax.axis_index(axis)
    return index % 2 == 0, index < lax.axis_size(axis) - 1, index > 0


def side_pair(values, e, port):
    upper = [v[:, 2 * e * port : (2 * e + 1) * port] for v in values]
    lower = [v[:, (2 * e + 1) * port : (2 * e + 2) * port] for v in values]
    return jnp.concatenate(upper, axis=1), jnp.concatenate(lower, axis=1)


def write_sends(values, port, match_ref, send_refs):
    at = 0
    for e, axis in enumerate(AXES):
        even, _, _ = parity_and_masks(axis)
        upper, lower = side_pair(values, e, port)
        outgoing = dot_nt(upper.astype(BF16), match_ref[e])
        lower = lower.astype(BF16).astype(F32)
        send_refs[at][...] = jnp.where(even, outgoing, lower).astype(BF16)
        at += 1
        if lax.axis_size(axis) > 2:
            send_refs[at][...] = jnp.where(even, lower, outgoing).astype(BF16)
            at += 1


def arrivals(recv_refs):
    at = 0
    out = []
    for axis in AXES:
        even, has_next, has_prev = parity_and_masks(axis)
        first = recv_refs[at][...].astype(F32)
        at += 1
        if lax.axis_size(axis) > 2:
            second = recv_refs[at][...].astype(F32)
            at += 1
            after, before = jnp.where(even, first, second), jnp.where(even, second, first)
        else:
            after, before = first, first
        after = jnp.where(has_next, after, 0.0)
        before = jnp.where(has_prev, before, 0.0)
        out.append((after, before, has_next, has_prev))
    return out


def exchange(sends):
    at = 0
    out = []
    for axis in AXES:
        size = lax.axis_size(axis)
        for first in (0, 1) if size > 2 else (0,):
            swaps = []
            for p in range(first, size - 1, 2):
                swaps += [(p, p + 1), (p + 1, p)]
            out.append(lax.ppermute(sends[at], axis, swaps))
            at += 1
    return out


def send_shapes(load_count, width):
    total = sum(2 if lax.axis_size(axis) > 2 else 1 for axis in AXES)
    return [shape_of((load_count, width), BF16) for _ in range(total)]


def own_terms(values, port):
    sides = []
    for axis in AXES:
        _, has_next, has_prev = parity_and_masks(axis)
        sides += [has_next, has_prev]
    out = []
    for v in values:
        parts = [
            jnp.where(sides[k], v[:, k * port : (k + 1) * port], 0.0) for k in range(len(sides))
        ]
        parts.append(jnp.zeros((v.shape[0], v.shape[1] - len(sides) * port), F32))
        out.append(jnp.concatenate(parts, axis=1))
    return out


def arrival_terms(recv_refs, match_ref, slot_total, port, nb):
    parts = [[] for _ in range(slot_total)]
    for e, (after, before, _, _) in enumerate(arrivals(recv_refs)):
        partner = dot(after.astype(BF16), match_ref[e])
        for s in range(slot_total):
            parts[s] += [partner[:, s * port : (s + 1) * port], before[:, s * port : (s + 1) * port]]
    out = []
    for s in range(slot_total):
        rest = nb - 2 * len(AXES) * port
        parts[s].append(jnp.zeros((parts[s][0].shape[0], rest), F32))
        out.append(jnp.concatenate(parts[s], axis=1))
    return out


def per_device(
    coupling_modes, mode_stiffness, boundary_stiffness, slot_type, partner_slot, port_map, loads
):
    modes = coupling_modes[0]
    nb = modes.shape[0]
    boundary = boundary_stiffness[0]
    rhs = loads[0, 0, 0]
    slot_total, _, load_count = rhs.shape
    kinds = slot_type[0, 0, 0]
    partners = partner_slot[0, 0, 0]
    ports = port_map[0, 0, 0]
    port = nb // SIDES
    block = 2 * port
    count = nb // block
    width = slot_total * port
    insts = lax.axis_size("inst")
    faces = lax.axis_size("face")
    vec = (slot_total, load_count, nb)

    stiffness = mode_stiffness[0][None, :]
    offs = [(i, j) for j in range(count) for i in range(j)]
    diag = [(i, i) for i in range(count)]
    middle = offs[1:-1]
    plan = [(offs[:1], False)]
    plan += [(middle[k : k + 2], False) for k in range(0, len(middle), 2)]
    plan += [(diag, True), (offs[-1:], False)]
    diag_at = len(plan) - 2

    def add(a, b):
        return (a.astype(F32) + b.astype(F32)).astype(BF16)

    z = lax.axis_index("face")
    inner = (z == 1) | (z == 2)
    line = faces == 4

    def tied(value, *others):
        return lax.optimization_barrier((value, *others))[0]

    def inward(part):
        return lax.ppermute(part, "face", [(0, 1), (3, 2)])

    def across(part):
        return lax.ppermute(part, "face", [(1, 2), (2, 1)])

    def outward(part):
        return lax.ppermute(part, "face", [(1, 0), (2, 3)])

    def modal(chunks, after, name):
        return modal_blocks(modes, stiffness, boundary, chunks, after, name)

    split = max(1, len(plan) - 2)
    part = modal(plan[:1], (), "modal_0")
    if line:
        got = [inward(part[0])]
    part += modal(plan[1:split], (), "modal_1")
    if line:
        got += [inward(p) for p in part[1:]]
        left = [add(part[0], tied(got[0], *part[1:]))]
        swapped = [across(left[0])]
    part += modal(plan[split:], tuple(left) if line else (), "modal_2")
    if line:
        left.append(add(part[1], tied(got[1], part[-1])))
        swapped.append(across(left[1]))
        got += [inward(tied(p, left[1])) for p in part[split:]]
        left.append(add(part[2], tied(got[2], left[1])))
        swapped.append(across(left[2]))
        total = [add(left[0], tied(swapped[0], left[2]))]
        spread = [outward(total[0])]
    ready = total[0] if line else part[-1]

    def prepare(loads_ref, partner_ref, ports_ref, _, b_ref, match_ref, back_ref, *send_refs):
        values = []
        for s in range(slot_total):
            b = loads_ref[s].T
            b_ref[s] = b
            values.append(b / theta)
        row = lax.broadcasted_iota(jnp.int32, (width, width), 0)
        for e in range(len(AXES)):
            target = jnp.concatenate(
                [partner_ref[e, s] * port + ports_ref[e, s : s + 1, :] for s in range(slot_total)],
                axis=1,
            )
            table = (row == target).astype(F32)
            match_ref[e] = table.astype(BF16)
            back_ref[e] = table.T.astype(BF16)
        write_sends(values, port, match_ref, send_refs)

    tables = shape_of((len(AXES), width, width), BF16)
    bt, match, back, *sends = call(
        prepare,
        [shape_of(vec, F32), tables, tables] + send_shapes(load_count, width),
        (rhs, partners, ports, ready),
        [VMEM, SMEM, VMEM, ANY],
        200_000_000,
        "prepare",
    )

    received = exchange(sends)

    if line:
        total.append(add(left[1], tied(swapped[1], *sends)))
        spread.append(outward(total[1]))
        for n in range(3, len(plan)):
            left.append(add(part[n], tied(got[n], total[1], left[-1])))
            swapped.append(across(left[n]))
        for n in range(2, len(plan)):
            total.append(add(left[n], tied(swapped[n], left[-1], total[-1])))
            spread.append(outward(total[n]))
        summed = [
            jnp.where(inner, t, tied(s, total[-1])) for t, s in zip(total, spread)
        ]
    else:
        summed = [lax.psum(p.astype(F32), "face").astype(BF16) for p in part]

    if insts == 2:
        candidates = [(own, lax.ppermute(own, "inst", [(0, 1), (1, 0)])) for own in summed]
    else:
        candidates = []
        for own in summed:
            stack = lax.all_gather(own, "inst", axis=0)
            candidates.append(
                tuple(
                    lax.dynamic_index_in_dim(stack, kinds[s], 0, keepdims=False)
                    for s in range(slot_total)
                )
            )
    options = len(candidates[0])
    candidates[diag_at] = tuple(unpack_diagonal(list(candidates[diag_at]), count))

    def each_option(kind_ref, use):
        me = lax.axis_index("inst")
        for s in range(slot_total):
            for option in range(options):
                if insts == 2:
                    hit = (kind_ref[s] == me) if option == 0 else (kind_ref[s] != me)
                    pl.when(hit)(lambda s=s, option=option: use(s, option))
                elif option == s:
                    use(s, option)

    def products(x, chunk_ids, chunk_refs):
        acc = [None] * count

        def gather(j, v):
            acc[j] = v if acc[j] is None else acc[j] + v

        cols = [x[:, i * block : (i + 1) * block] for i in range(count)]
        for n, ref in zip(chunk_ids, chunk_refs):
            pairs, packed = plan[n]
            for at, (i, j) in enumerate(pairs):
                if packed:
                    gather(i, dot(cols[i], ref[i]))
                else:
                    matrix = ref[at * block : (at + 1) * block, :]
                    gather(j, dot(cols[i], matrix))
                    gather(i, dot_nt(cols[j], matrix))
        return acc

    everything = list(range(len(plan)))
    flops_all = 2 * slot_total * load_count * nb * nb

    def matrices(ids):
        return [candidates[n][o] for o in range(options) for n in ids]

    def option_refs(refs, ids, option):
        return refs[option * len(ids) : (option + 1) * len(ids)]


    def couple_first(b_ref, match_ref, _, *refs):
        out_ref = refs[-1]
        values = [b_ref[s] / theta for s in range(slot_total)]
        mine = own_terms(values, port)
        theirs = arrival_terms(refs[:-1], match_ref, slot_total, port, nb)
        for s in range(slot_total):
            out_ref[s] = b_ref[s] - mine[s] + theirs[s]

    r1_base = call(
        couple_first,
        shape_of(vec, F32),
        (bt, match, total[-1] if line else part[-1], *received),
        [VMEM, VMEM, ANY] + [VMEM] * len(received),
        50_000_000,
        "couple_first",
    )

    early, late = everything[:-1], everything[-1:]

    def first_product(b_ref, r_ref, kind_ref, *refs):
        out_ref = refs[-1]

        def use(s, option):
            x = (b_ref[s] / theta).astype(BF16)
            acc = products(x, early, option_refs(refs, early, option))
            for j in range(count):
                cols = slice(j * block, (j + 1) * block)
                out_ref[s, :, cols] = r_ref[s, :, cols] - acc[j]

        each_option(kind_ref, use)

    mats = matrices(early)
    r1_part = call(
        first_product,
        shape_of(vec, F32),
        (bt, r1_base, kinds, *mats),
        [VMEM, VMEM, SMEM] + [VMEM] * len(mats),
        flops_all,
        "first_product",
    )

    def first_finish(b_ref, r_ref, match_ref, kind_ref, *refs):
        refs, (r_out, d_out), send_refs = (
            refs[: options * len(late)],
            refs[options * len(late) : options * len(late) + 2],
            refs[options * len(late) + 2 :],
        )

        def use(s, option):
            x = (b_ref[s] / theta).astype(BF16)
            acc = products(x, late, option_refs(refs, late, option))
            for j in range(count):
                cols = slice(j * block, (j + 1) * block)
                r = r_ref[s, :, cols]
                if acc[j] is not None:
                    r = r - acc[j]
                r_out[s, :, cols] = r
                d_out[s, :, cols] = keep[0] * (b_ref[s, :, cols] / theta) + gain[0] * r

        each_option(kind_ref, use)
        write_sends([d_out[s] for s in range(slot_total)], port, match_ref, send_refs)

    mats = matrices(late)
    r1, d1, *sends = call(
        first_finish,
        [shape_of(vec, F32), shape_of(vec, F32)] + send_shapes(load_count, width),
        (bt, r1_part, match, kinds, *mats),
        [VMEM, VMEM, VMEM, SMEM] + [VMEM] * len(mats),
        flops_all // 4,
        "first_finish",
    )

    received = exchange(sends)
    mats = matrices(everything)

    def second_product(d_ref, r_ref, kind_ref, *refs):
        out_ref = refs[-1]

        def use(s, option):
            d = d_ref[s]
            acc = products(d.astype(BF16), everything, option_refs(refs, everything, option))
            base = r_ref[s] - own_terms([d], port)[0]
            for j in range(count):
                cols = slice(j * block, (j + 1) * block)
                out_ref[s, :, cols] = base[:, cols] - acc[j]

        each_option(kind_ref, use)

    r2_base = call(
        second_product,
        shape_of(vec, F32),
        (d1, r1, kinds, *mats),
        [VMEM, VMEM, SMEM] + [VMEM] * len(mats),
        flops_all,
        "second_product",
    )

    def second_finish(d_ref, r_ref, match_ref, *refs):
        total = len(received)
        recv_refs, r_out, d_out, send_refs = (
            refs[:total],
            refs[total],
            refs[total + 1],
            refs[total + 2 :],
        )
        theirs = arrival_terms(recv_refs, match_ref, slot_total, port, nb)
        values = []
        for s in range(slot_total):
            r = r_ref[s] + theirs[s]
            d = keep[1] * d_ref[s] + gain[1] * r
            r_out[s] = r
            d_out[s] = d
            values.append(d)
        write_sends(values, port, match_ref, send_refs)

    r2, d2, *sends = call(
        second_finish,
        [shape_of(vec, F32), shape_of(vec, F32)] + send_shapes(load_count, width),
        (d1, r2_base, match, *received),
        [VMEM] * (3 + len(received)),
        100_000_000,
        "second_finish",
    )

    received = exchange(sends)

    def third_product(b_ref, d1_ref, d_ref, r_ref, kind_ref, *refs):
        out_ref = refs[-1]

        def use(s, option):
            d = d_ref[s]
            acc = products(d.astype(BF16), everything, option_refs(refs, everything, option))
            base = r_ref[s] - own_terms([d], port)[0]
            sums = (b_ref[s] / theta + d1_ref[s]) + d
            for j in range(count):
                cols = slice(j * block, (j + 1) * block)
                last = keep[2] * d[:, cols] + gain[2] * (base[:, cols] - acc[j])
                out_ref[s, cols, :] = (sums[:, cols] + last).T

        each_option(kind_ref, use)

    x_base = call(
        third_product,
        shape_of(rhs.shape, F32),
        (bt, d1, d2, r2, kinds, *mats),
        [VMEM] * 4 + [SMEM] + [VMEM] * len(mats),
        flops_all,
        "third_product",
    )

    def third_finish(x_ref, back_ref, *refs):
        out_ref = refs[-1]
        row = lax.broadcasted_iota(jnp.int32, (width, width), 0)
        col = lax.broadcasted_iota(jnp.int32, (width, width), 1)
        unit = (row == col).astype(F32).astype(BF16)
        for e, (after, before, _, _) in enumerate(arrivals(refs[:-1])):
            partner = dot_nt(back_ref[e], after.astype(BF16))
            behind = dot_nt(unit, before.astype(BF16))
            for s in range(slot_total):
                for side, term in ((2 * e, partner), (2 * e + 1, behind)):
                    rows = slice(side * port, (side + 1) * port)
                    out_ref[s, rows, :] = (
                        x_ref[s, rows, :] + gain[2] * term[s * port : (s + 1) * port]
                    )
        for s in range(slot_total):
            rows = slice(2 * len(AXES) * port, nb)
            out_ref[s, rows, :] = x_ref[s, rows, :]

    displacement = call(
        third_finish,
        shape_of(rhs.shape, F32),
        (x_base, back, *received),
        [VMEM] * (2 + len(received)),
        100_000_000,
        "third_finish",
    )
    return displacement[None, None, None]


def solution(mesh):
    placed = (
        P(("types", "inst"), None, "face"),
        P(("types", "inst"), "face"),
        P(("types", "inst"), "face", None),
        P("types", "inst", "face", None),
        P("types", "inst", "face", None, None),
        P("types", "inst", "face", None, None, None),
        P("types", "inst", "face", None, None, None),
    )
    return jax.shard_map(
        per_device,
        mesh=mesh,
        in_specs=placed,
        out_specs=P("types", "inst", "face", None, None, None),
        check_vma=False,
    )
```

```python
import jax
import jax.numpy as jnp
from jax import lax
from jax.experimental import pallas as pl
from jax.experimental.pallas import tpu as pltpu
from jax.sharding import PartitionSpec as P

SIDES = 8
lower_bound = 2.0
upper_bound = 12.0
theta = (upper_bound + lower_bound) / 2.0
delta = (upper_bound - lower_bound) / 2.0
sigma = theta / delta
w0 = 1.0 / sigma
w1 = 1.0 / (2.0 * sigma - w0)
w2 = 1.0 / (2.0 * sigma - w1)
w3 = 1.0 / (2.0 * sigma - w2)
keep = (w1 * w0, w2 * w1, w3 * w2)
gain = (2.0 * w1 / delta, 2.0 * w2 / delta, 2.0 * w3 / delta)

AXES = ("inst", "face", "types")
F32 = jnp.float32
BF16 = jnp.bfloat16
VMEM = pl.BlockSpec(memory_space=pltpu.VMEM)
ANY = pl.BlockSpec(memory_space=pl.ANY)
HBM = pl.BlockSpec(memory_space=pltpu.HBM)
LIMIT = 12 * 2**20
GRANT = 61 * 2**20
SMEM = pl.BlockSpec(memory_space=pltpu.SMEM)


def dot(a, b):
    return lax.dot_general(a, b, (((1,), (0,)), ((), ())), preferred_element_type=F32)


def dot_nt(a, b):
    return lax.dot_general(a, b, (((1,), (1,)), ((), ())), preferred_element_type=F32)


def shape_of(dims, dtype):
    return jax.ShapeDtypeStruct(dims, dtype)


def call(body, out_shape, operands, specs, flops, name):
    moved = sum(x.size * x.dtype.itemsize for x in operands)
    return pl.pallas_call(
        body,
        out_shape=out_shape,
        in_specs=specs,
        out_specs=jax.tree.map(lambda _: VMEM, out_shape),
        cost_estimate=pl.CostEstimate(flops=flops, bytes_accessed=moved, transcendentals=0),
        compiler_params=pltpu.CompilerParams(vmem_limit_bytes=LIMIT),
        name=name,
    )(*operands)


def owned_boundary(b_ref, row, height, col, width, face):
    held = b_ref.shape[0]
    step = min(held, height)
    parts = []
    for start in range(row, row + height, step):
        local = b_ref[start % held : start % held + step, col : col + width]
        parts.append(jnp.where(face == start // held, local, 0.0))
    return parts[0] if len(parts) == 1 else jnp.concatenate(parts, axis=0)


def modal_blocks(modes, stiffness, boundary, chunk, line, after, name):
    nb, depth = modes.shape
    block = 2 * nb // SIDES
    half = block // 2
    count = nb // block
    ktile = block
    load = min(1024, depth)
    loads = depth // load
    every = [pair for pairs, _ in chunk for pair in pairs]
    rows = sorted({i for pair in every for i in pair})
    lefts = sorted({i for i, _ in every})
    phases = [every[k : k + count] for k in range(0, len(every), count)]
    extra = 16 * ((2 * count + 15) // 16)
    tail = extra if any(packed for _, packed in chunk) else 0
    full = max(2 if packed else len(pairs) for pairs, packed in chunk)
    out_rows = full * block + tail

    def body(modes_ref, stiff_ref, bound_ref, *refs):
        keep_ref, send_ref = refs[len(after) : len(after) + 2]
        row_ref, left_ref, inverse, b_ref, acc_ref, sems = refs[len(after) + 2 :]
        stiff_copy = pltpu.make_async_copy(stiff_ref, inverse, sems.at[0])
        bound_copy = pltpu.make_async_copy(bound_ref, b_ref, sems.at[1])
        stiff_copy.start()
        copies = {}
        for n in range(loads):
            cols = pl.ds(n * load, load)
            for at, i in enumerate(rows):
                copies[i, n] = pltpu.make_async_copy(
                    modes_ref.at[pl.ds(i * block, block), cols],
                    row_ref.at[at, :, cols],
                    sems.at[2 + n * len(rows) + at],
                )
                copies[i, n].start()
        bound_copy.start()
        stiff_copy.wait()
        inverse[...] = 1.0 / inverse[...]
        face = lax.axis_index("face")
        scaled_done = set()

        def multiply(*accs):
            for p, pairs in enumerate(phases):
                columns = sorted({j for _, j in pairs})
                for n in range(depth // ktile):
                    cols = pl.ds(n * ktile, ktile)
                    for i in sorted({i for pair in pairs for i in pair}):
                        copy = copies.pop((i, n * ktile // load), None)
                        if copy is not None:
                            copy.wait()
                    for i in sorted({i for i, _ in pairs}):
                        if (i, n) not in scaled_done:
                            scaled_done.add((i, n))
                            value = row_ref[rows.index(i), :, cols].astype(F32)
                            left_ref[lefts.index(i), :, cols] = (
                                value * inverse[:, cols]
                            ).astype(BF16)
                    q = n % 2
                    for at, j in enumerate(columns):
                        register = (n // 2 * len(columns) + at) % 2
                        pltpu.matmul_push_rhs(
                            row_ref[rows.index(j), :, cols],
                            staging_register=register,
                            mxu_index=q,
                            transpose=True,
                        )
                        fresh = register
                        for m, (i, jj) in enumerate(pairs):
                            if jj == j:
                                pltpu.matmul_acc_lhs(
                                    accs[2 * m + q],
                                    left_ref[lefts.index(i), :, cols],
                                    load_staged_rhs=fresh,
                                )
                                fresh = None
                for m in range(len(pairs)):
                    acc_ref[p * count + m] = pltpu.matmul_pop(accs[2 * m]) + pltpu.matmul_pop(
                        accs[2 * m + 1]
                    )
            bound_copy.wait()
            base = 0
            parts = []
            for pairs, packed in chunk:
                sums = [acc_ref[base + m] for m in range(len(pairs))]
                base += len(pairs)
                parts.append((packed_values if packed else plain_values)(pairs, sums))
            first_kept = ((face == 0) | (face == 3)) if line else True
            for n in range(full + (tail > 0)):
                lines = slice(n * block, n * block + (block if n < full else tail))
                a, b = [
                    part[n] if n < len(part) else jnp.zeros((lines.stop - lines.start, block), F32)
                    for part in parts
                ]
                keep_ref[lines, :] = jnp.where(first_kept, a, b).astype(BF16)
                send_ref[lines, :] = jnp.where(first_kept, b, a).astype(BF16)

        def plain_values(pairs, sums):
            return [
                owned_boundary(b_ref, i * block, block, j * block, block, face) - total
                for (i, j), total in zip(pairs, sums)
            ]

        def packed_values(pairs, sums):
            r = lax.broadcasted_iota(jnp.int32, (half, half), 0)
            c = lax.broadcasted_iota(jnp.int32, (half, half), 1)
            rr = lax.broadcasted_iota(jnp.int32, (block, block), 0)
            cc = lax.broadcasted_iota(jnp.int32, (block, block), 1)
            highs, rests, both, offs = [], [], [], []
            for (i, _), total in zip(pairs, sums):
                mine = owned_boundary(b_ref, i * block, block, i * block, block, face)
                diff = mine - total
                own = jnp.sum(jnp.where(rr == cc, mine, 0.0), axis=0, keepdims=True)
                modal = jnp.sum(jnp.where(rr == cc, total, 0.0), axis=0, keepdims=True)
                high = own.astype(BF16).astype(F32)
                highs.append(high)
                rests.append((own - high) - modal)
                a = diff[:half, :half]
                b = diff[half:, half:]
                both.append(jnp.where(r < c, a, jnp.where(r > c, b, 0.0)))
                offs.append(diff[:half, half:])
            fill = [jnp.zeros((extra - 2 * count, block), F32)] if extra > 2 * count else []
            return [squared(both), squared(offs), jnp.concatenate(highs + rests + fill, axis=0)]

        def squared(tiles):
            pairs = [tiles[n : n + 2] for n in range(0, len(tiles), 2)]
            return jnp.concatenate([jnp.concatenate(two, axis=1) for two in pairs], axis=0)

        pl.run_scoped(
            multiply,
            *[pltpu.ACC(q)((block, block), F32) for _ in phases[0] for q in (0, 1)],
        )

    return pl.pallas_call(
        body,
        out_shape=[shape_of((out_rows, block), BF16)] * 2,
        in_specs=[ANY] * (3 + len(after)),
        out_specs=[VMEM] * 2,
        scratch_shapes=[
            pltpu.VMEM((len(rows), block, depth), BF16),
            pltpu.VMEM((len(lefts), block, depth), BF16),
            pltpu.VMEM((1, depth), F32),
            pltpu.VMEM(boundary.shape, F32),
            pltpu.VMEM((len(every), block, block), F32),
            pltpu.SemaphoreType.DMA((2 + loads * len(rows),)),
        ],
        cost_estimate=pl.CostEstimate(
            flops=2 * len(every) * block * block * depth,
            bytes_accessed=2 * len(rows) * block * depth,
            transcendentals=0,
        ),
        compiler_params=pltpu.CompilerParams(vmem_limit_bytes=GRANT),
        name=name,
    )(modes, stiffness, boundary, *after)


def unpack_diagonal(packed_list, part, count):
    block = packed_list[0].shape[2]
    half = block // 2

    def body(*refs):
        total = len(refs) // 2
        r = lax.broadcasted_iota(jnp.int32, (half, half), 0)
        c = lax.broadcasted_iota(jnp.int32, (half, half), 1)
        for p_ref, d_ref in zip(refs[:total], refs[total:]):
            lines = p_ref[part, 2 * block :, :].astype(F32)
            for i in range(count):
                line = lines[i : i + 1, :] + lines[count + i : count + i + 1, :]
                top, side = half * (i // 2), half * (i % 2)
                both = p_ref[part, top : top + half, side : side + half].astype(F32)
                off = p_ref[part, block + top : block + top + half, side : side + half]
                upper = jnp.where(r < c, both, 0.0)
                lower = jnp.where(r > c, both, 0.0)
                a = upper + upper.T + jnp.where(r == c, line[:, :half], 0.0)
                b = lower + lower.T + jnp.where(r == c, line[:, half:], 0.0)
                d_ref[i, :half, :half] = a.astype(BF16)
                d_ref[i, half:, half:] = b.astype(BF16)
                d_ref[i, :half, half:] = off
                d_ref[i, half:, :half] = off.astype(F32).T.astype(BF16)

    return call(
        body,
        [shape_of((count, block, block), BF16) for _ in packed_list],
        packed_list,
        [VMEM] * len(packed_list),
        10_000_000,
        "unpack_diagonal",
    )


def parity_and_masks(axis):
    index = lax.axis_index(axis)
    return index % 2 == 0, index < lax.axis_size(axis) - 1, index > 0


def side_pair(values, e, port):
    upper = [v[:, 2 * e * port : (2 * e + 1) * port] for v in values]
    lower = [v[:, (2 * e + 1) * port : (2 * e + 2) * port] for v in values]
    return jnp.concatenate(upper, axis=1), jnp.concatenate(lower, axis=1)


def write_sends(values, port, match_ref, send_refs):
    at = 0
    for e, axis in enumerate(AXES):
        even, _, _ = parity_and_masks(axis)
        upper, lower = side_pair(values, e, port)
        outgoing = dot_nt(upper.astype(BF16), match_ref[e])
        lower = lower.astype(BF16).astype(F32)
        send_refs[at][...] = jnp.where(even, outgoing, lower).astype(BF16)
        at += 1
        if lax.axis_size(axis) > 2:
            send_refs[at][...] = jnp.where(even, lower, outgoing).astype(BF16)
            at += 1


def arrivals(recv_refs):
    at = 0
    out = []
    for axis in AXES:
        even, has_next, has_prev = parity_and_masks(axis)
        first = recv_refs[at][...].astype(F32)
        at += 1
        if lax.axis_size(axis) > 2:
            second = recv_refs[at][...].astype(F32)
            at += 1
            after, before = jnp.where(even, first, second), jnp.where(even, second, first)
        else:
            after, before = first, first
        after = jnp.where(has_next, after, 0.0)
        before = jnp.where(has_prev, before, 0.0)
        out.append((after, before, has_next, has_prev))
    return out


def exchange(sends, skip=()):
    at = 0
    out = []
    for axis in AXES:
        size = lax.axis_size(axis)
        for first in (0, 1) if size > 2 else (0,):
            swaps = []
            for p in range(first, size - 1, 2):
                swaps += [(p, p + 1), (p + 1, p)]
            out.append(None if axis in skip else lax.ppermute(sends[at], axis, swaps))
            at += 1
    return out


def pairings():
    return [
        (axis, first)
        for axis in AXES
        for first in ((0, 1) if lax.axis_size(axis) > 2 else (0,))
    ]


def send_shapes(load_count, width):
    total = sum(2 if lax.axis_size(axis) > 2 else 1 for axis in AXES)
    return [shape_of((load_count, width), BF16) for _ in range(total)]


def own_terms(values, port):
    sides = []
    for axis in AXES:
        _, has_next, has_prev = parity_and_masks(axis)
        sides += [has_next, has_prev]
    out = []
    for v in values:
        parts = [
            jnp.where(sides[k], v[:, k * port : (k + 1) * port], 0.0) for k in range(len(sides))
        ]
        parts.append(jnp.zeros((v.shape[0], v.shape[1] - len(sides) * port), F32))
        out.append(jnp.concatenate(parts, axis=1))
    return out


def arrival_terms(recv_refs, match_ref, slot_total, port, nb):
    parts = [[] for _ in range(slot_total)]
    for e, (after, before, _, _) in enumerate(arrivals(recv_refs)):
        partner = dot(after.astype(BF16), match_ref[e])
        for s in range(slot_total):
            parts[s] += [partner[:, s * port : (s + 1) * port], before[:, s * port : (s + 1) * port]]
    out = []
    for s in range(slot_total):
        rest = nb - 2 * len(AXES) * port
        parts[s].append(jnp.zeros((parts[s][0].shape[0], rest), F32))
        out.append(jnp.concatenate(parts[s], axis=1))
    return out


def per_device(
    coupling_modes, mode_stiffness, boundary_stiffness, slot_type, partner_slot, port_map, loads
):
    modes = coupling_modes[0]
    nb = modes.shape[0]
    boundary = boundary_stiffness[0]
    rhs = loads[0, 0, 0]
    slot_total, _, load_count = rhs.shape
    kinds = slot_type[0, 0, 0]
    partners = partner_slot[0, 0, 0]
    ports = port_map[0, 0, 0]
    port = nb // SIDES
    block = 2 * port
    count = nb // block
    width = slot_total * port
    insts = lax.axis_size("inst")
    faces = lax.axis_size("face")
    vec = (slot_total, load_count, nb)

    stiffness = mode_stiffness[0][None, :]
    offs = [(i, j) for j in range(count) for i in range(j)]
    diag = [(i, i) for i in range(count)]
    tail_pairs = [(0, count - 1), (count - 2, count - 1)]
    middle = [pair for pair in offs[2:] if pair not in tail_pairs]
    plan = [
        ((offs[:1], False), (offs[1:2], False)),
        ((diag, True), (middle, False)),
        ((tail_pairs[:1], False), (tail_pairs[1:], False)),
    ]

    def add(a, b):
        return (a.astype(F32) + b.astype(F32)).astype(BF16)

    z = lax.axis_index("face")
    line = faces == 4
    outer = (z == 0) | (z == 3)

    def tied(value, *others):
        return lax.optimization_barrier((value, *others))[0]

    def beside(part):
        return lax.ppermute(part, "face", [(0, 1), (1, 0), (2, 3), (3, 2)])

    def across(part):
        return lax.ppermute(part, "face", [(0, 3), (3, 0), (1, 2), (2, 1)])

    def modal(n, *after):
        return modal_blocks(modes, stiffness, boundary, plan[n], line, after, f"modal_{n}")

    keep_0, send_0 = modal(0)
    if line:
        got_0 = beside(send_0)
    keep_1, send_1 = modal(1)
    if line:
        got_1 = beside(send_1)
        left_0 = add(keep_0, tied(got_0, keep_1))
        swap_0 = across(left_0)
    keep_2, send_2 = modal(2, *([left_0] if line else []))
    if line:
        got_2 = beside(send_2)
        left_1 = add(keep_1, tied(got_1, keep_2))
        swap_1 = across(left_1)
    ready = left_1 if line else keep_2

    def prepare(loads_ref, partner_ref, ports_ref, _, b_ref, match_ref, back_ref, *send_refs):
        values = []
        for s in range(slot_total):
            b = loads_ref[s].T
            b_ref[s] = b
            values.append(b / theta)
        row = lax.broadcasted_iota(jnp.int32, (width, width), 0)
        for e in range(len(AXES)):
            target = jnp.concatenate(
                [partner_ref[e, s] * port + ports_ref[e, s : s + 1, :] for s in range(slot_total)],
                axis=1,
            )
            table = (row == target).astype(F32)
            match_ref[e] = table.astype(BF16)
            back_ref[e] = table.T.astype(BF16)
        write_sends(values, port, match_ref, send_refs)

    tables = shape_of((len(AXES), width, width), BF16)
    bt, match, back, *sends = call(
        prepare,
        [shape_of(vec, F32), tables, tables] + send_shapes(load_count, width),
        (rhs, partners, ports, ready),
        [VMEM, SMEM, VMEM, ANY],
        200_000_000,
        "prepare",
    )

    if line:
        near, far = [n for n, (axis, _) in enumerate(pairings()) if axis == "face"]
        received = exchange(sends, ("face",))
        total_0 = add(left_0, tied(swap_0, *sends))
        high = total_0.shape[0]
        spread = beside(jnp.concatenate([total_0, sends[near]], axis=0))
        spread_0, received[near] = spread[:high], spread[high:]
        left_2 = add(keep_2, tied(got_2, total_0))
        high = left_2.shape[0]
        swap_2 = across(jnp.concatenate([left_2, sends[far]], axis=0))
        total_1 = add(left_1, tied(swap_1, left_2))
        spread_1 = beside(total_1)
        total_2 = add(left_2, tied(swap_2[:high], total_1))
        received[far] = swap_2[high:]
        spread_2 = beside(total_2)
        late = (tied(spread_0, total_2), tied(spread_1, total_2), spread_2)
        summed = [
            jnp.stack([jnp.where(outer, t, s), jnp.where(outer, s, t)])
            for t, s in zip((total_0, total_1, total_2), late)
        ]
        after_sums = total_2
    else:
        received = exchange(sends)
        summed = [
            jnp.stack([lax.psum(half.astype(F32), "face").astype(BF16) for half in halves])
            for halves in ((keep_0, send_0), (keep_1, send_1), (keep_2, send_2))
        ]
        after_sums = summed[-1]

    if insts == 2:
        candidates = [(own, lax.ppermute(own, "inst", [(0, 1), (1, 0)])) for own in summed]
    else:
        candidates = []
        for own in summed:
            stack = lax.all_gather(own, "inst", axis=0)
            candidates.append(
                tuple(
                    lax.dynamic_index_in_dim(stack, kinds[s], 0, keepdims=False)
                    for s in range(slot_total)
                )
            )
    options = len(candidates[0])
    diagonals = unpack_diagonal(list(candidates[1]), 0, count)

    def each_option(kind_ref, use):
        me = lax.axis_index("inst")
        for s in range(slot_total):
            for option in range(options):
                if insts == 2:
                    hit = (kind_ref[s] == me) if option == 0 else (kind_ref[s] != me)
                    pl.when(hit)(lambda s=s, option=option: use(s, option))
                elif option == s:
                    use(s, option)

    def products(x, chunk_ids, chunk_refs):
        acc = [None] * count

        def gather(j, v):
            acc[j] = v if acc[j] is None else acc[j] + v

        cols = [x[:, i * block : (i + 1) * block] for i in range(count)]
        for n, ref in zip(chunk_ids, chunk_refs):
            if n == len(plan):
                for i in range(count):
                    gather(i, dot(cols[i], ref[i]))
                continue
            for part, (pairs, packed) in enumerate(plan[n]):
                for at, (i, j) in enumerate([] if packed else pairs):
                    matrix = ref[part, at * block : (at + 1) * block, :]
                    gather(j, dot(cols[i], matrix))
                    gather(i, dot_nt(cols[j], matrix))
        return acc

    candidates.append(tuple(diagonals))
    everything = [0, 1, len(plan), 2]
    flops_all = 2 * slot_total * load_count * nb * nb

    def matrices(ids):
        return [candidates[n][o] for o in range(options) for n in ids]

    def option_refs(refs, ids, option):
        return refs[option * len(ids) : (option + 1) * len(ids)]


    def couple_first(b_ref, match_ref, _, *refs):
        out_ref = refs[-1]
        values = [b_ref[s] / theta for s in range(slot_total)]
        mine = own_terms(values, port)
        theirs = arrival_terms(refs[:-1], match_ref, slot_total, port, nb)
        for s in range(slot_total):
            out_ref[s] = b_ref[s] - mine[s] + theirs[s]

    r1_base = call(
        couple_first,
        shape_of(vec, F32),
        (bt, match, after_sums, *received),
        [VMEM, VMEM, ANY] + [VMEM] * len(received),
        50_000_000,
        "couple_first",
    )

    early, late = everything[:-1], everything[-1:]

    def first_product(b_ref, r_ref, kind_ref, *refs):
        out_ref = refs[-1]

        def use(s, option):
            x = (b_ref[s] / theta).astype(BF16)
            acc = products(x, early, option_refs(refs, early, option))
            for j in range(count):
                cols = slice(j * block, (j + 1) * block)
                out_ref[s, :, cols] = r_ref[s, :, cols] - acc[j]

        each_option(kind_ref, use)

    mats = matrices(early)
    r1_part = call(
        first_product,
        shape_of(vec, F32),
        (bt, r1_base, kinds, *mats),
        [VMEM, VMEM, SMEM] + [VMEM] * len(mats),
        flops_all,
        "first_product",
    )

    def first_finish(b_ref, r_ref, match_ref, kind_ref, *refs):
        refs, (r_out, d_out), send_refs = (
            refs[: options * len(late)],
            refs[options * len(late) : options * len(late) + 2],
            refs[options * len(late) + 2 :],
        )

        def use(s, option):
            x = (b_ref[s] / theta).astype(BF16)
            acc = products(x, late, option_refs(refs, late, option))
            for j in range(count):
                cols = slice(j * block, (j + 1) * block)
                r = r_ref[s, :, cols]
                if acc[j] is not None:
                    r = r - acc[j]
                r_out[s, :, cols] = r
                d_out[s, :, cols] = keep[0] * (b_ref[s, :, cols] / theta) + gain[0] * r

        each_option(kind_ref, use)
        write_sends([d_out[s] for s in range(slot_total)], port, match_ref, send_refs)

    mats = matrices(late)
    r1, d1, *sends = call(
        first_finish,
        [shape_of(vec, F32), shape_of(vec, F32)] + send_shapes(load_count, width),
        (bt, r1_part, match, kinds, *mats),
        [VMEM, VMEM, VMEM, SMEM] + [VMEM] * len(mats),
        flops_all // 4,
        "first_finish",
    )

    received = exchange(sends)
    mats = matrices(everything)

    def second_product(d_ref, r_ref, kind_ref, *refs):
        out_ref = refs[-1]

        def use(s, option):
            d = d_ref[s]
            acc = products(d.astype(BF16), everything, option_refs(refs, everything, option))
            base = r_ref[s] - own_terms([d], port)[0]
            for j in range(count):
                cols = slice(j * block, (j + 1) * block)
                out_ref[s, :, cols] = base[:, cols] - acc[j]

        each_option(kind_ref, use)

    r2_base = call(
        second_product,
        shape_of(vec, F32),
        (d1, r1, kinds, *mats),
        [VMEM, VMEM, SMEM] + [VMEM] * len(mats),
        flops_all,
        "second_product",
    )

    def second_finish(d_ref, r_ref, match_ref, *refs):
        total = len(received)
        recv_refs, r_out, d_out, send_refs = (
            refs[:total],
            refs[total],
            refs[total + 1],
            refs[total + 2 :],
        )
        theirs = arrival_terms(recv_refs, match_ref, slot_total, port, nb)
        values = []
        for s in range(slot_total):
            r = r_ref[s] + theirs[s]
            d = keep[1] * d_ref[s] + gain[1] * r
            r_out[s] = r
            d_out[s] = d
            values.append(d)
        write_sends(values, port, match_ref, send_refs)

    r2, d2, *sends = call(
        second_finish,
        [shape_of(vec, F32), shape_of(vec, F32)] + send_shapes(load_count, width),
        (d1, r2_base, match, *received),
        [VMEM] * (3 + len(received)),
        100_000_000,
        "second_finish",
    )

    received = exchange(sends)

    def third_product(b_ref, d1_ref, d_ref, r_ref, kind_ref, *refs):
        out_ref = refs[-1]

        def use(s, option):
            d = d_ref[s]
            acc = products(d.astype(BF16), everything, option_refs(refs, everything, option))
            base = r_ref[s] - own_terms([d], port)[0]
            sums = (b_ref[s] / theta + d1_ref[s]) + d
            for j in range(count):
                cols = slice(j * block, (j + 1) * block)
                last = keep[2] * d[:, cols] + gain[2] * (base[:, cols] - acc[j])
                out_ref[s, cols, :] = (sums[:, cols] + last).T

        each_option(kind_ref, use)

    x_base = call(
        third_product,
        shape_of(rhs.shape, F32),
        (bt, d1, d2, r2, kinds, *mats),
        [VMEM] * 4 + [SMEM] + [VMEM] * len(mats),
        flops_all,
        "third_product",
    )

    def third_finish(x_ref, back_ref, *refs):
        out_ref = refs[-1]
        row = lax.broadcasted_iota(jnp.int32, (width, width), 0)
        col = lax.broadcasted_iota(jnp.int32, (width, width), 1)
        unit = (row == col).astype(F32).astype(BF16)
        for e, (after, before, _, _) in enumerate(arrivals(refs[:-1])):
            partner = dot_nt(back_ref[e], after.astype(BF16))
            behind = dot_nt(unit, before.astype(BF16))
            for s in range(slot_total):
                for side, term in ((2 * e, partner), (2 * e + 1, behind)):
                    rows = slice(side * port, (side + 1) * port)
                    out_ref[s, rows, :] = (
                        x_ref[s, rows, :] + gain[2] * term[s * port : (s + 1) * port]
                    )
        for s in range(slot_total):
            rows = slice(2 * len(AXES) * port, nb)
            out_ref[s, rows, :] = x_ref[s, rows, :]

    displacement = call(
        third_finish,
        shape_of(rhs.shape, F32),
        (x_base, back, *received),
        [VMEM] * (2 + len(received)),
        100_000_000,
        "third_finish",
    )
    return displacement[None, None, None]


def solution(mesh):
    placed = (
        P(("types", "inst"), None, "face"),
        P(("types", "inst"), "face"),
        P(("types", "inst"), "face", None),
        P("types", "inst", "face", None),
        P("types", "inst", "face", None, None),
        P("types", "inst", "face", None, None, None),
        P("types", "inst", "face", None, None, None),
    )
    return jax.shard_map(
        per_device,
        mesh=mesh,
        in_specs=placed,
        out_specs=P("types", "inst", "face", None, None, None),
        check_vma=False,
    )
```
